32 devices in a mesh: shard: 32 (over z, y, x, core).
Axes of the slice: x: 2, y: 2, z: 4, core: 2. Of those that a mesh axis runs over, the one named last changes fastest.
Arguments:
- weights_master: float32 [262144], P('shard'), may hold values from -6 to 6
- first_moment: float32 [262144], P('shard'), may hold values from -1.2 to 1.2
- second_moment: float32 [262144], P('shard'), may hold values from 0.005 to 0.5
- grad_one: float32 [262144], P('shard'), may hold values from -140 to 140
- grad_two: float32 [262144], P('shard'), may hold values from -140 to 140
Outputs:
- gathered_one: bfloat16 [262144], replicated
- gathered_two: bfloat16 [262144], replicated
- master_out: float32 [262144], P('shard')
- first_out: float32 [262144], P('shard')
- second_out: float32 [262144], P('shard')
The draws below stay inside these ranges and needn't reach their ends.
All inputs are finite; a program needn't handle non-finite values.
Results may differ from the reference program's by a relative error of at most 0.001.
Values may be sent and summed in bfloat16 or wider, within the bound.
A program may use at most 64 MiB of HBM per device.

```python
import math
import jax
import jax.numpy as jnp

PER_DEV = 8192
PARAMS = 262144
STEP0 = 100
N_SHARD = 32


def gradient_draw(key, salt):
    key = jax.random.fold_in(key, salt)
    key_base, key_block = jax.random.split(key, 2)
    blocks = PARAMS // 128
    device = (jnp.arange(PARAMS) // PER_DEV).astype(jnp.float32)
    fraction = device / (N_SHARD - 1)
    block_scale = jnp.exp(jax.random.uniform(key_block, (blocks,), jnp.float32, 0.0, math.log(10.0)))
    block_scale = jnp.repeat(block_scale, 128)
    base_value = jnp.clip(jax.random.normal(key_base, (PARAMS,), jnp.float32), -4.0, 4.0)
    ramp_up = 1.0 + 2.0 * fraction
    return base_value * block_scale * ramp_up


def draw_grad_one(key, part):
    return gradient_draw(key, 11)


def draw_grad_two(key, part):
    return gradient_draw(key, 23)


def block_levels(rng, dims, cuts, smallest, top_value):
    gain = 1.0
    for position, parts in cuts:
        steps = jax.random.uniform(jax.random.fold_in(jax.random.fold_in(rng, 6), position), (parts,), jnp.float32, smallest / len(cuts), top_value / len(cuts))
        gain = gain * jnp.repeat(jnp.exp(steps), dims[position] // parts).reshape((-1,) + (1,) * (len(dims) - 1 - position))
    return gain


def scatter_about(own_key, dims, deviation, limit, cuts=(), held_as=jnp.bfloat16):
    entries = jax.random.normal(own_key, dims, jnp.float32) * deviation
    if len(cuts) > 0:
        entries = block_levels(own_key, dims, cuts, -0.22, 0.18) * entries
    return jnp.clip(entries, min=-limit, max=limit).astype(held_as)


def setup_inputs(seed: int = 0) -> dict:
    streams_of = jax.random.split(jax.random.key(seed), 6)
    return {
        "weights_master": scatter_about(streams_of[0], (PARAMS,), 1.0, 6.0, ((0, 32),), jnp.float32),
        "first_moment": scatter_about(streams_of[1], (PARAMS,), 0.2, 1.2, ((0, 32),), jnp.float32),
        "second_moment": jnp.clip(jnp.exp(math.log(0.5) - 4.6051702 * jax.random.uniform(streams_of[2], (PARAMS,), jnp.float32) ** block_levels(streams_of[2], (PARAMS,), ((0, 32),), -0.2, 0.2)), 0.005, 0.5),
        "grad_one": draw_grad_one(jax.random.fold_in(streams_of[5], 71), 0),
        "grad_two": draw_grad_two(jax.random.fold_in(streams_of[5], 71), 0),
    }


def square_sum(gradient):
    return jnp.sum(gradient * gradient)

def adam_update(weights, moment_one, moment_two, gradient, total_sq, param_count, step_index):
    clip_limit = 0.25 * math.sqrt(param_count)
    factor = jnp.minimum(1.0, clip_limit / (jnp.sqrt(total_sq) + 1e-06))
    clipped = factor * gradient
    moment_one = 0.9 * moment_one + 0.1 * clipped
    moment_two = 0.95 * moment_two + 0.05 * clipped * clipped
    bias_first = 1.0 - 0.9 ** (STEP0 + step_index)
    bias_second = 1.0 - 0.95 ** (STEP0 + step_index)
    direction = moment_one / bias_first / (jnp.sqrt(moment_two / bias_second) + 1e-08)
    weights = weights - 0.02 * (direction + 0.1 * weights)
    return (weights, moment_one, moment_two)

def reference(weights_master, first_moment, second_moment, grad_one, grad_two):
    weights, moment_one, moment_two = adam_update(weights_master, first_moment, second_moment, grad_one, square_sum(grad_one), PARAMS, 1)
    gathered_one = weights.astype(jnp.bfloat16)
    weights, moment_one, moment_two = adam_update(weights, moment_one, moment_two, grad_two, square_sum(grad_two), PARAMS, 2)
    gathered_two = weights.astype(jnp.bfloat16)
    return (gathered_one, gathered_two, weights, moment_one, moment_two)
```

```python
import functools
import math

import jax
import jax.numpy as jnp
from jax import lax
from jax.experimental import pallas as pl
from jax.experimental.pallas import tpu as pltpu
from jax.sharding import PartitionSpec as P

STEP0 = 100
LANES = 128
PLANE = 8
MESH = pl.DeviceIdType.MESH


def adam_update(weights, moment_one, moment_two, gradient, total_sq, param_count, step_index):
    clip_limit = 0.25 * math.sqrt(param_count)
    factor = jnp.minimum(1.0, clip_limit / (jnp.sqrt(total_sq) + 1e-06))
    clipped = factor * gradient
    moment_one = 0.9 * moment_one + 0.1 * clipped
    moment_two = 0.95 * moment_two + 0.05 * clipped * clipped
    scale_first = 1.0 / (1.0 - 0.9 ** (STEP0 + step_index))
    scale_second = 1.0 / (1.0 - 0.95 ** (STEP0 + step_index))
    direction = moment_one * scale_first / (jnp.sqrt(moment_two * scale_second) + 1e-08)
    weights = weights - 0.02 * (direction + 0.1 * weights)
    return (weights, moment_one, moment_two)


def far_peers(z, depth):
    if depth == 4:
        half = z // 2
        return [z + 1 - 2 * (z % 2), 2 - half, 3 - 3 * half]
    return [lax.rem(z + k, depth) for k in range(1, depth)]


def exchange_kernel(
    n,
    w_hbm, m_hbm, v_hbm, g1_hbm, g2_hbm,
    one_ref, two_ref, w_out, m_out, v_out,
    w_in, m_in, v_in, g1_in, g2_in, sums,
    in_sem, sum_send, sum_recv, send_sem, far_recv, first_recv, second_recv, pair_recv,
):
    me = lax.axis_index("shard")
    depth = n // PLANE
    z, q = me // PLANE, me % PLANE
    y, x, c = q // 4, (q // 2) % 2, q % 2

    def at(z_, y_, x_, c_):
        return ((z_ * 2 + y_) * 2 + x_) * 2 + c_

    zs = far_peers(z, depth)
    plane_peers = [z * PLANE + (q + k) % PLANE for k in range(1, PLANE)]
    z_peers = [p * PLANE + q for p in zs]
    pair = at(z, y, x, 1 - c)
    along_y = at(z, 1 - y, x, c)
    along_x = at(z, y, 1 - x, c)

    barrier = pltpu.get_barrier_semaphore()
    for peer in reversed(plane_peers + z_peers):
        pl.semaphore_signal(barrier, inc=1, device_id=(peer,), device_id_type=MESH)

    loads = [
        pltpu.make_async_copy(src, dst, in_sem.at[i])
        for i, (src, dst) in enumerate(
            [(g1_hbm, g1_in), (g2_hbm, g2_in), (w_hbm, w_in), (m_hbm, m_in), (v_hbm, v_in)]
        )
    ]
    for load in loads:
        load.start()
    loads[0].wait()
    loads[1].wait()
    grad_one, grad_two = g1_in[...], g2_in[...]
    sums[z, q, pl.ds(0, 1), :] = jnp.sum(grad_one * grad_one, axis=0, keepdims=True)
    sums[z, q, pl.ds(1, 1), :] = jnp.sum(grad_two * grad_two, axis=0, keepdims=True)
    for load in loads[2:]:
        load.wait()

    pl.semaphore_wait(barrier, len(plane_peers) + len(z_peers))

    def remote(src, dst, send, recv, peer):
        return pltpu.make_async_remote_copy(
            src_ref=src, dst_ref=dst, send_sem=send, recv_sem=recv,
            device_id=(peer,), device_id_type=MESH,
        )

    own = sums.at[z, q]
    for peer in plane_peers:
        remote(own, own, sum_send.at[0], sum_recv.at[0], peer).start()
    others = sums.at[0, pl.ds(0, PLANE - 1)]
    remote(others, others, sum_send.at[0], sum_recv.at[0], pair).wait_recv()
    plane = sums.at[z]
    for peer in reversed(z_peers):
        remote(plane, plane, sum_send.at[1], sum_recv.at[1], peer).start()
    rest = sums.at[pl.ds(0, depth - 1)]
    remote(rest, rest, sum_send.at[1], sum_recv.at[1], pair).wait_recv()

    totals = jnp.sum(jnp.sum(sums[...], axis=(0, 1)), axis=1, keepdims=True)
    param_count = n * w_in.shape[0] * LANES
    weights, moment_one, moment_two = adam_update(
        w_in[...], m_in[...], v_in[...], grad_one, totals[0:1], param_count, 1
    )
    one_ref[me] = weights.astype(jnp.bfloat16)
    weights, moment_one, moment_two = adam_update(
        weights, moment_one, moment_two, grad_two, totals[1:2], param_count, 2
    )
    two_ref[me] = weights.astype(jnp.bfloat16)
    w_out[...] = weights
    m_out[...] = moment_one
    v_out[...] = moment_two

    halves = [one_ref, two_ref]
    near = [along_y, along_x]
    last = [along_x, along_y]

    def block(h, index):
        return halves[h].at[index]

    def to_far(h, index, peer):
        remote(block(h, index), block(h, index), send_sem.at[h], far_recv.at[h, z], peer).start()

    def to_near(h, index, z_):
        remote(block(h, index), block(h, index), send_sem.at[h], first_recv.at[h, z_], near[h]).start()

    def to_last(h, index, slot):
        remote(block(h, index), block(h, index), send_sem.at[h], second_recv.at[h, slot], last[h]).start()

    def to_pair(h, index):
        remote(block(h, index), block(h, index), send_sem.at[h], pair_recv.at[h], pair).start()

    def arrived(h, index, sem):
        remote(block(h, index), block(h, index), send_sem.at[h], sem, pair).wait_recv()

    turned = [(1 - y, x), (y, 1 - x)]
    opposite = [(y, 1 - x), (1 - y, x)]
    both = [(1 - y, 1 - x), (1 - y, 1 - x)]

    for peer in reversed(z_peers):
        for h in range(2):
            to_far(h, me, peer)
    for h in range(2):
        to_near(h, me, z)
        to_last(h, me, 2 * z)
        to_pair(h, me)

    def from_near(z_):
        for h in range(2):
            index = at(z_, *turned[h], c)
            arrived(h, index, first_recv.at[h, z_])
            to_last(h, index, 2 * z_ + 1)
            to_pair(h, index)

    def from_last(z_, s):
        for h in range(2):
            index = at(z_, *(opposite, both)[s][h], c)
            arrived(h, index, second_recv.at[h, 2 * z_ + s])
            to_pair(h, index)

    from_near(z)
    for p in zs:
        for h in range(2):
            index = at(p, y, x, c)
            arrived(h, index, far_recv.at[h, p])
            to_near(h, index, p)
            to_last(h, index, 2 * p)
            to_pair(h, index)
    from_last(z, 0)
    for p in zs:
        from_near(p)
    from_last(z, 1)
    for p in zs:
        from_last(p, 0)
    for p in zs:
        from_last(p, 1)

    remote(others, others, sum_send.at[0], sum_recv.at[0], pair).wait_send()
    remote(rest, rest, sum_send.at[1], sum_recv.at[1], pair).wait_send()
    for h in range(2):
        half = halves[h].at[pl.ds(0, n // 2)]
        remote(half, half, send_sem.at[h], pair_recv.at[h], pair).wait_recv()
    for h in range(2):
        sent = halves[h].at[pl.ds(0, n - 1)]
        remote(sent, sent, send_sem.at[h], pair_recv.at[h], pair).wait_send()


def store_kernel(count, *refs):
    sems = refs[-1]
    copies = [
        pltpu.make_async_copy(refs[i], refs[count + i], sems.at[i]) for i in range(count)
    ]
    for copy in copies:
        copy.start()
    for copy in copies:
        copy.wait()


def on_device(weights_master, first_moment, second_moment, grad_one, grad_two):
    n = lax.axis_size("shard")
    rows = weights_master.shape[0] // LANES
    depth = n // PLANE
    flat = [a.reshape(rows, LANES) for a in (weights_master, first_moment, second_moment, grad_one, grad_two)]
    shapes = [((n, rows, LANES), jnp.bfloat16)] * 2 + [((rows, LANES), jnp.float32)] * 3
    any_spec = pl.BlockSpec(memory_space=pl.ANY)
    vmem_spec = pl.BlockSpec(memory_space=pltpu.VMEM)
    results = pl.pallas_call(
        functools.partial(exchange_kernel, n),
        out_shape=[pltpu.VMEM(s, d) for s, d in shapes],
        in_specs=[any_spec] * 5,
        out_specs=[vmem_spec] * 5,
        scratch_shapes=[pltpu.VMEM((rows, LANES), jnp.float32)] * 5
        + [
            pltpu.VMEM((depth, PLANE, 2, LANES), jnp.float32),
            pltpu.SemaphoreType.DMA((5,)),
            pltpu.SemaphoreType.DMA((2,)),
            pltpu.SemaphoreType.DMA((2,)),
            pltpu.SemaphoreType.DMA((2,)),
            pltpu.SemaphoreType.DMA((2, depth)),
            pltpu.SemaphoreType.DMA((2, depth)),
            pltpu.SemaphoreType.DMA((2, 2 * depth)),
            pltpu.SemaphoreType.DMA((2,)),
        ],
        compiler_params=pltpu.CompilerParams(
            collective_id=0, has_side_effects=True, vmem_limit_bytes=rows * LANES * 4 * 5 + (2 << 20)
        ),
        name="exchange",
    )(*flat)
    stored = pl.pallas_call(
        functools.partial(store_kernel, 5),
        out_shape=[jax.ShapeDtypeStruct(s, d) for s, d in shapes],
        in_specs=[any_spec] * 5,
        out_specs=[any_spec] * 5,
        scratch_shapes=[pltpu.SemaphoreType.DMA((5,))],
        compiler_params=pltpu.CompilerParams(vmem_limit_bytes=1 << 20),
        name="store",
    )(*results)
    return tuple(a.reshape(-1) for a in stored)


def solution(mesh):
    return jax.shard_map(
        on_device,
        mesh=mesh,
        in_specs=(P("shard"), P("shard"), P("shard"), P("shard"), P("shard")),
        out_specs=(P(), P(), P("shard"), P("shard"), P("shard")),
        check_vma=False,
    )
```

```python
import functools
import math

import jax
import jax.numpy as jnp
from jax import lax
from jax.experimental import pallas as pl
from jax.experimental.pallas import tpu as pltpu
from jax.sharding import PartitionSpec as P

STEP0 = 100
LANES = 128
PLANE = 8
VMEM_BYTES = 67043328
MESH = pl.DeviceIdType.MESH


def adam_update(weights, moment_one, moment_two, gradient, total_sq, param_count, step_index):
    clip_limit = 0.25 * math.sqrt(param_count)
    factor = jnp.minimum(1.0, clip_limit / (jnp.sqrt(total_sq) + 1e-06))
    clipped = factor * gradient
    moment_one = 0.9 * moment_one + 0.1 * clipped
    moment_two = 0.95 * moment_two + 0.05 * clipped * clipped
    scale_first = 1.0 / (1.0 - 0.9 ** (STEP0 + step_index))
    scale_second = 1.0 / (1.0 - 0.95 ** (STEP0 + step_index))
    direction = moment_one * scale_first / (jnp.sqrt(moment_two * scale_second) + 1e-08)
    weights = weights - 0.02 * (direction + 0.1 * weights)
    return (weights, moment_one, moment_two)


def far_peers(z, depth):
    if depth == 4:
        half = z // 2
        return [z + 1 - 2 * (z % 2), 2 - half, 3 - 3 * half]
    return [lax.rem(z + k, depth) for k in range(1, depth)]


def exchange_kernel(
    n,
    w_hbm, m_hbm, v_hbm, g1_hbm, g2_hbm,
    one_ref, two_ref, w_out, m_out, v_out,
    w_in, m_in, v_in, g1_in, g2_in, sums,
    in_sem, sum_sem, send_sem, far_recv, first_recv, second_recv, pair_recv,
):
    me = lax.axis_index("shard")
    depth = n // PLANE
    z, q = me // PLANE, me % PLANE
    y, x, c = q // 4, (q // 2) % 2, q % 2

    def at(z_, y_, x_, c_):
        return ((z_ * 2 + y_) * 2 + x_) * 2 + c_

    zs = far_peers(z, depth)
    z_peers = [p * PLANE + q for p in zs]
    pair = at(z, y, x, 1 - c)
    along_y = at(z, 1 - y, x, c)
    along_x = at(z, y, 1 - x, c)

    everyone = [(me + k) % n for k in range(1, n)]
    barrier = pltpu.get_barrier_semaphore()
    for peer in everyone:
        pl.semaphore_signal(barrier, inc=1, device_id=(peer,), device_id_type=MESH)

    loads = [
        pltpu.make_async_copy(src, dst, in_sem.at[i])
        for i, (src, dst) in enumerate(
            [(g1_hbm, g1_in), (g2_hbm, g2_in), (w_hbm, w_in), (m_hbm, m_in), (v_hbm, v_in)]
        )
    ]
    for load in loads:
        load.start()
    loads[0].wait()
    loads[1].wait()
    grad_one, grad_two = g1_in[...], g2_in[...]
    sums[me, pl.ds(0, 1), :] = jnp.sum(grad_one * grad_one, axis=0, keepdims=True)
    sums[me, pl.ds(1, 1), :] = jnp.sum(grad_two * grad_two, axis=0, keepdims=True)
    for load in loads[2:]:
        load.wait()

    pl.semaphore_wait(barrier, n - 1)

    def remote(src, dst, send, recv, peer):
        return pltpu.make_async_remote_copy(
            src_ref=src, dst_ref=dst, send_sem=send, recv_sem=recv,
            device_id=(peer,), device_id_type=MESH,
        )

    own = sums.at[me]
    for peer in everyone:
        remote(own, own, sum_sem.at[0], sum_sem.at[1], peer).start()
    others = sums.at[pl.ds(0, n - 1)]
    all_sums = remote(others, others, sum_sem.at[0], sum_sem.at[1], pair)
    all_sums.wait_recv()

    totals = jnp.sum(jnp.sum(sums[...], axis=0), axis=1, keepdims=True)
    param_count = n * w_in.shape[0] * LANES
    weights, moment_one, moment_two = adam_update(
        w_in[...], m_in[...], v_in[...], grad_one, totals[0:1], param_count, 1
    )
    one_ref[me] = weights.astype(jnp.bfloat16)
    weights, moment_one, moment_two = adam_update(
        weights, moment_one, moment_two, grad_two, totals[1:2], param_count, 2
    )
    two_ref[me] = weights.astype(jnp.bfloat16)
    w_out[...] = weights
    m_out[...] = moment_one
    v_out[...] = moment_two

    halves = [one_ref, two_ref]
    diag = at(z, 1 - y, 1 - x, c)
    near = [along_y, along_x]
    last = [along_x, along_y]

    def block(h, index):
        return halves[h].at[index]

    def to_far(h, index, peer):
        remote(block(h, index), block(h, index), send_sem.at[h], far_recv.at[h, z], peer).start()

    def to_near(h, index, z_):
        remote(block(h, index), block(h, index), send_sem.at[h], first_recv.at[h, z_], near[h]).start()

    def to_last(h, index, slot):
        remote(block(h, index), block(h, index), send_sem.at[h], second_recv.at[h, slot], last[h]).start()
        remote(block(h, index), block(h, index), send_sem.at[h], second_recv.at[h, slot + 1], diag).start()

    def to_pair(h, index):
        remote(block(h, index), block(h, index), send_sem.at[h], pair_recv.at[h], pair).start()

    def arrived(h, index, sem):
        remote(block(h, index), block(h, index), send_sem.at[h], sem, pair).wait_recv()

    turned = [(1 - y, x), (y, 1 - x)]
    opposite = [(y, 1 - x), (1 - y, x)]
    both = [(1 - y, 1 - x), (1 - y, 1 - x)]

    for peer in reversed(z_peers):
        for h in range(2):
            to_far(h, me, peer)
    for h in range(2):
        to_near(h, me, z)
        to_last(h, me, 2 * z)
        to_pair(h, me)

    def from_near(z_):
        for h in range(2):
            index = at(z_, *turned[h], c)
            arrived(h, index, first_recv.at[h, z_])
            to_pair(h, index)

    def from_last(z_, s):
        for h in range(2):
            index = at(z_, *(opposite, both)[s][h], c)
            arrived(h, index, second_recv.at[h, 2 * z_ + s])
            to_pair(h, index)

    from_near(z)
    for p in zs:
        for h in range(2):
            index = at(p, y, x, c)
            arrived(h, index, far_recv.at[h, p])
            to_near(h, index, p)
            to_last(h, index, 2 * p)
            to_pair(h, index)
    from_last(z, 0)
    for p in zs:
        from_near(p)
    from_last(z, 1)
    for p in zs:
        from_last(p, 0)
    for p in zs:
        from_last(p, 1)

    all_sums.wait_send()
    for h in range(2):
        half = halves[h].at[pl.ds(0, n // 2)]
        remote(half, half, send_sem.at[h], pair_recv.at[h], pair).wait_recv()
    for h in range(2):
        sent = halves[h].at[pl.ds(0, n - 1)]
        remote(sent, sent, send_sem.at[h], pair_recv.at[h], pair).wait_send()


def store_kernel(count, *refs):
    sems = refs[-1]
    copies = [
        pltpu.make_async_copy(refs[i], refs[count + i], sems.at[i]) for i in range(count)
    ]
    for copy in copies:
        copy.start()
    for copy in copies:
        copy.wait()


def on_device(weights_master, first_moment, second_moment, grad_one, grad_two):
    n = lax.axis_size("shard")
    rows = weights_master.shape[0] // LANES
    depth = n // PLANE
    flat = [a.reshape(rows, LANES) for a in (weights_master, first_moment, second_moment, grad_one, grad_two)]
    shapes = [((n, rows, LANES), jnp.bfloat16)] * 2 + [((rows, LANES), jnp.float32)] * 3
    any_spec = pl.BlockSpec(memory_space=pl.ANY)
    vmem_spec = pl.BlockSpec(memory_space=pltpu.VMEM)
    held = sum(math.prod(s) * jnp.dtype(d).itemsize for s, d in shapes)
    grant = min(60 * 1024 * 1024, VMEM_BYTES - held - (1 << 20))
    results = pl.pallas_call(
        functools.partial(exchange_kernel, n),
        out_shape=[pltpu.VMEM(s, d) for s, d in shapes],
        in_specs=[any_spec] * 5,
        out_specs=[vmem_spec] * 5,
        scratch_shapes=[pltpu.VMEM((rows, LANES), jnp.float32)] * 5
        + [
            pltpu.VMEM((n, 2, LANES), jnp.float32),
            pltpu.SemaphoreType.DMA((5,)),
            pltpu.SemaphoreType.DMA((2,)),
            pltpu.SemaphoreType.DMA((2,)),
            pltpu.SemaphoreType.DMA((2, depth)),
            pltpu.SemaphoreType.DMA((2, depth)),
            pltpu.SemaphoreType.DMA((2, 2 * depth)),
            pltpu.SemaphoreType.DMA((2,)),
        ],
        compiler_params=pltpu.CompilerParams(
            collective_id=0, has_side_effects=True, vmem_limit_bytes=grant
        ),
        name="exchange",
    )(*flat)
    stored = pl.pallas_call(
        functools.partial(store_kernel, 5),
        out_shape=[jax.ShapeDtypeStruct(s, d) for s, d in shapes],
        in_specs=[any_spec] * 5,
        out_specs=[any_spec] * 5,
        scratch_shapes=[pltpu.SemaphoreType.DMA((5,))],
        compiler_params=pltpu.CompilerParams(vmem_limit_bytes=1 << 20),
        name="store",
    )(*results)
    return tuple(a.reshape(-1) for a in stored)


def solution(mesh):
    return jax.shard_map(
        on_device,
        mesh=mesh,
        in_specs=(P("shard"), P("shard"), P("shard"), P("shard"), P("shard")),
        out_specs=(P(), P(), P("shard"), P("shard"), P("shard")),
        check_vma=False,
    )
```

```python
import functools
import math

import jax
import jax.numpy as jnp
from jax import lax
from jax.experimental import pallas as pl
from jax.experimental.pallas import tpu as pltpu
from jax.sharding import PartitionSpec as P

STEP0 = 100
LANES = 128
PLANE = 8
VMEM_BYTES = 67043328
MESH = pl.DeviceIdType.MESH


def adam_update(weights, moment_one, moment_two, gradient, total_sq, param_count, step_index):
    clip_limit = 0.25 * math.sqrt(param_count)
    factor = jnp.minimum(1.0, clip_limit / (jnp.sqrt(total_sq) + 1e-06))
    clipped = factor * gradient
    moment_one = 0.9 * moment_one + 0.1 * clipped
    moment_two = 0.95 * moment_two + 0.05 * clipped * clipped
    scale_first = 1.0 / (1.0 - 0.9 ** (STEP0 + step_index))
    scale_second = 1.0 / (1.0 - 0.95 ** (STEP0 + step_index))
    direction = moment_one * scale_first / (jnp.sqrt(moment_two * scale_second) + 1e-08)
    weights = weights - 0.02 * (direction + 0.1 * weights)
    return (weights, moment_one, moment_two)


def far_peers(z, depth):
    if depth == 4:
        half = z // 2
        return [z + 1 - 2 * (z % 2), 2 - half, 3 - 3 * half]
    return [lax.rem(z + k, depth) for k in range(1, depth)]


def exchange_kernel(
    n,
    w_hbm, m_hbm, v_hbm, g1_hbm, g2_hbm,
    one_ref, two_ref, w_out, m_out, v_out,
    w_in, m_in, v_in, g1_in, g2_in, sums,
    in_sem, sum_sem, send_sem, far_recv, first_recv, second_recv, pair_recv,
):
    me = lax.axis_index("shard")
    depth = n // PLANE
    z, q = me // PLANE, me % PLANE
    y, x, c = q // 4, (q // 2) % 2, q % 2

    def at(z_, y_, x_, c_):
        return ((z_ * 2 + y_) * 2 + x_) * 2 + c_

    zs = far_peers(z, depth)
    z_peers = [p * PLANE + q for p in zs]
    pair = at(z, y, x, 1 - c)
    along_y = at(z, 1 - y, x, c)
    along_x = at(z, y, 1 - x, c)

    everyone = [p * PLANE + (q + k) % PLANE for p in zs[::-1] for k in reversed(range(PLANE))]
    everyone += [z * PLANE + (q + k) % PLANE for k in range(1, PLANE)]
    barrier = pltpu.get_barrier_semaphore()
    for peer in everyone:
        pl.semaphore_signal(barrier, inc=1, device_id=(peer,), device_id_type=MESH)

    loads = [
        pltpu.make_async_copy(src, dst, in_sem.at[i])
        for i, (src, dst) in enumerate(
            [(g1_hbm, g1_in), (g2_hbm, g2_in), (w_hbm, w_in), (m_hbm, m_in), (v_hbm, v_in)]
        )
    ]
    for load in loads:
        load.start()
    loads[0].wait()
    loads[1].wait()
    grad_one, grad_two = g1_in[...], g2_in[...]
    sums[me, pl.ds(0, 1), :] = jnp.sum(grad_one * grad_one, axis=0, keepdims=True)
    sums[me, pl.ds(1, 1), :] = jnp.sum(grad_two * grad_two, axis=0, keepdims=True)
    for load in loads[2:]:
        load.wait()

    pl.semaphore_wait(barrier, n - 1)

    def remote(src, dst, send, recv, peer):
        return pltpu.make_async_remote_copy(
            src_ref=src, dst_ref=dst, send_sem=send, recv_sem=recv,
            device_id=(peer,), device_id_type=MESH,
        )

    own = sums.at[me]
    for peer in everyone:
        remote(own, own, sum_sem.at[0], sum_sem.at[1], peer).start()
    others = sums.at[pl.ds(0, n - 1)]
    all_sums = remote(others, others, sum_sem.at[0], sum_sem.at[1], pair)
    all_sums.wait_recv()

    totals = jnp.sum(jnp.sum(sums[...], axis=0), axis=1, keepdims=True)
    param_count = n * w_in.shape[0] * LANES
    weights, moment_one, moment_two = adam_update(
        w_in[...], m_in[...], v_in[...], grad_one, totals[0:1], param_count, 1
    )
    one_ref[me] = weights.astype(jnp.bfloat16)
    weights, moment_one, moment_two = adam_update(
        weights, moment_one, moment_two, grad_two, totals[1:2], param_count, 2
    )
    two_ref[me] = weights.astype(jnp.bfloat16)
    w_out[...] = weights
    m_out[...] = moment_one
    v_out[...] = moment_two

    halves = [one_ref, two_ref]
    diag = at(z, 1 - y, 1 - x, c)
    near = [along_y, along_x]
    last = [along_x, along_y]

    def block(h, index):
        return halves[h].at[index]

    def to_far(h, index, peer):
        remote(block(h, index), block(h, index), send_sem.at[h], far_recv.at[h, z], peer).start()

    def to_near(h, index, z_):
        remote(block(h, index), block(h, index), send_sem.at[h], first_recv.at[h, z_], near[h]).start()

    def to_last(h, index, slot):
        remote(block(h, index), block(h, index), send_sem.at[h], second_recv.at[h, slot], last[h]).start()
        remote(block(h, index), block(h, index), send_sem.at[h], second_recv.at[h, slot + 1], diag).start()

    def to_pair(h, index):
        remote(block(h, index), block(h, index), send_sem.at[h], pair_recv.at[h], pair).start()

    def arrived(h, index, sem):
        remote(block(h, index), block(h, index), send_sem.at[h], sem, pair).wait_recv()

    turned = [(1 - y, x), (y, 1 - x)]
    opposite = [(y, 1 - x), (1 - y, x)]
    both = [(1 - y, 1 - x), (1 - y, 1 - x)]

    for peer in reversed(z_peers):
        for h in range(2):
            to_far(h, me, peer)
    for h in range(2):
        to_near(h, me, z)
        to_last(h, me, 2 * z)
        to_pair(h, me)

    def from_near(z_):
        for h in range(2):
            index = at(z_, *turned[h], c)
            arrived(h, index, first_recv.at[h, z_])
            to_pair(h, index)

    def from_last(z_, s):
        for h in range(2):
            index = at(z_, *(opposite, both)[s][h], c)
            arrived(h, index, second_recv.at[h, 2 * z_ + s])
            to_pair(h, index)

    for p in zs:
        for h in range(2):
            index = at(p, y, x, c)
            arrived(h, index, far_recv.at[h, p])
            to_near(h, index, p)
            to_last(h, index, 2 * p)
            to_pair(h, index)
    from_near(z)
    from_last(z, 0)
    for p in zs:
        from_near(p)
    from_last(z, 1)
    for p in zs:
        from_last(p, 0)
    for p in zs:
        from_last(p, 1)

    all_sums.wait_send()
    for h in range(2):
        half = halves[h].at[pl.ds(0, n // 2)]
        remote(half, half, send_sem.at[h], pair_recv.at[h], pair).wait_recv()
    for h in range(2):
        sent = halves[h].at[pl.ds(0, n - 1)]
        remote(sent, sent, send_sem.at[h], pair_recv.at[h], pair).wait_send()


def store_kernel(count, *refs):
    sems = refs[-1]
    copies = [
        pltpu.make_async_copy(refs[i], refs[count + i], sems.at[i]) for i in range(count)
    ]
    for copy in copies:
        copy.start()
    for copy in copies:
        copy.wait()


def on_device(weights_master, first_moment, second_moment, grad_one, grad_two):
    n = lax.axis_size("shard")
    rows = weights_master.shape[0] // LANES
    depth = n // PLANE
    flat = [a.reshape(rows, LANES) for a in (weights_master, first_moment, second_moment, grad_one, grad_two)]
    shapes = [((n, rows, LANES), jnp.bfloat16)] * 2 + [((rows, LANES), jnp.float32)] * 3
    any_spec = pl.BlockSpec(memory_space=pl.ANY)
    vmem_spec = pl.BlockSpec(memory_space=pltpu.VMEM)
    held = sum(math.prod(s) * jnp.dtype(d).itemsize for s, d in shapes)
    grant = min(60 * 1024 * 1024, VMEM_BYTES - held - (1 << 20))
    results = pl.pallas_call(
        functools.partial(exchange_kernel, n),
        out_shape=[pltpu.VMEM(s, d) for s, d in shapes],
        in_specs=[any_spec] * 5,
        out_specs=[vmem_spec] * 5,
        scratch_shapes=[pltpu.VMEM((rows, LANES), jnp.float32)] * 5
        + [
            pltpu.VMEM((n, 2, LANES), jnp.float32),
            pltpu.SemaphoreType.DMA((5,)),
            pltpu.SemaphoreType.DMA((2,)),
            pltpu.SemaphoreType.DMA((2,)),
            pltpu.SemaphoreType.DMA((2, depth)),
            pltpu.SemaphoreType.DMA((2, depth)),
            pltpu.SemaphoreType.DMA((2, 2 * depth)),
            pltpu.SemaphoreType.DMA((2,)),
        ],
        compiler_params=pltpu.CompilerParams(
            collective_id=0, has_side_effects=True, vmem_limit_bytes=grant
        ),
        name="exchange",
    )(*flat)
    stored = pl.pallas_call(
        functools.partial(store_kernel, 5),
        out_shape=[jax.ShapeDtypeStruct(s, d) for s, d in shapes],
        in_specs=[any_spec] * 5,
        out_specs=[any_spec] * 5,
        scratch_shapes=[pltpu.SemaphoreType.DMA((5,))],
        compiler_params=pltpu.CompilerParams(vmem_limit_bytes=1 << 20),
        name="store",
    )(*results)
    return tuple(a.reshape(-1) for a in stored)


def solution(mesh):
    return jax.shard_map(
        on_device,
        mesh=mesh,
        in_specs=(P("shard"), P("shard"), P("shard"), P("shard"), P("shard")),
        out_specs=(P(), P(), P("shard"), P("shard"), P("shard")),
        check_vma=False,
    )
```
